32 devices in a mesh: ep: 8 (over z, x), tp: 4 (over y, core).
Axes of the slice: x: 2, y: 2, z: 4, core: 2. Of those that a mesh axis runs over, the one named last changes fastest.
Arguments:
- tokens: bfloat16 [1024, 3072], P('ep', 'tp'), may hold values from -6 to 6
- expert_ids: int32 [1024, 2], P('ep'), may hold values from 0 to 7, all different within a row
- route_share: float32 [1024], P('ep'), may hold values from 0.5 to 0.95
- w_gate: bfloat16 [65536, 3072], P(('ep', 'tp')), may hold values from -0.109375 to 0.109375
- w_up: bfloat16 [65536, 3072], P(('ep', 'tp')), may hold values from -0.109375 to 0.109375
- w_down: bfloat16 [65536, 3072], P(('ep', 'tp')), may hold values from -0.0625 to 0.0625
- reward_head: float32 [3072], P('tp'), may hold values from -0.109375 to 0.109375
- upstream: bfloat16 [1024, 3072], P('ep', 'tp'), may hold values from -4 to 4
- pair_order: int32 [16], replicated, may hold values from 0 to 15, each once
Outputs:
- layer_out: bfloat16 [1024, 3072], P('ep', 'tp')
- rewards: float32 [16], replicated
- pair_loss: float32 [], replicated
- grad_tokens: bfloat16 [1024, 3072], P('ep', 'tp')
- grad_gate: bfloat16 [65536, 3072], P(('ep', 'tp'))
- grad_up: bfloat16 [65536, 3072], P(('ep', 'tp'))
- grad_down: bfloat16 [65536, 3072], P(('ep', 'tp'))
The draws below stay inside these ranges and needn't reach their ends.
Inputs may be any that keep to these rules, and one draw needn't show every extreme that they name: `expert_ids`: each row names 2 different experts. `pair_order`: each of the 16 sequence indices appears once.
All inputs are finite; a program needn't handle non-finite values.
Results may differ from the reference program's by a relative error of at most 0.014.
Values may be sent and summed in bfloat16 or wider, within the bound.
A program may use at most 128 MiB of HBM per device.

```python
import math
from functools import partial
import jax
import jax.numpy as jnp
from jax import lax

D = 3072
FF = 8192
EXPERTS = 8
TOPK = 2
SEQ_LEN = 64
TOK_DEV = 128
TOKENS = 1024
SEQS = 16
N_EP = 8
N_TP = 4


def shard_levels(own_key, extent, shards, smallest, high):
    factor_of = 1.0
    for axis_at, blocks in shards:
        draws = jax.random.uniform(jax.random.fold_in(jax.random.fold_in(own_key, 6), axis_at), (blocks,), jnp.float32, smallest / len(shards), high / len(shards))
        factor_of = factor_of * jnp.repeat(jnp.exp(draws), extent[axis_at] // blocks).reshape((-1,) + (1,) * (len(extent) - 1 - axis_at))
    return factor_of


def choose_distinct(own_key, rows, count, top, lift):
    sequence = jax.random.permutation(jax.random.fold_in(own_key, 1), count)
    favour = sequence
    for power in range(3):
        favour = favour * favour // count
    favour = favour * lift // count
    lots = jax.random.randint(jax.random.fold_in(own_key, 2), (rows, count), 0, 4096) + favour
    fixed_rows = jax.random.permutation(jax.random.fold_in(own_key, 3), rows)[jnp.arange(count) % rows]
    lots = jnp.where(jnp.arange(rows)[:, None] == fixed_rows[None, :], 1 << 14, lots)
    score = lots * count + jnp.arange(count)
    return lax.top_k(score.astype(jnp.int32), top)[1].astype(jnp.int32)


def centred(rng, extent, deviation, most, split=(), kind=jnp.bfloat16):
    gain = shard_levels(rng, extent, split, -0.22, 0.18) if split else 1.0
    entries = jax.random.normal(rng, extent, jnp.float32) * deviation * gain
    return jnp.minimum(jnp.maximum(entries, -most), most).astype(kind)


def setup_inputs(seed: int = 0) -> dict:
    seeds = jax.random.split(jax.random.key(seed), 10)
    return {
        "tokens": centred(seeds[0], (TOKENS, D), 1.0, 6.0, ((0, 8), (1, 4))),
        "expert_ids": choose_distinct(seeds[1], TOKENS, EXPERTS, TOPK, 2048),
        "route_share": jnp.clip(0.5 + 0.45 * jax.random.uniform(seeds[2], (TOKENS,), jnp.float32) ** shard_levels(seeds[2], (TOKENS,), ((0, 8),), -0.2, 0.2), 0.5, 0.95),
        "w_gate": centred(seeds[3], (EXPERTS * FF, D), D ** -0.5, 0.109375, ((0, 32),)),
        "w_up": centred(seeds[4], (EXPERTS * FF, D), D ** -0.5, 0.109375, ((0, 32),)),
        "w_down": centred(seeds[5], (EXPERTS * FF, D), FF ** -0.5, 0.0625, ((0, 32),)),
        "reward_head": centred(seeds[6], (D,), D ** -0.5, 0.109375, ((0, 4),), jnp.float32),
        "upstream": centred(seeds[7], (TOKENS, D), 0.5, 4.0, ((0, 8), (1, 4))),
        "pair_order": jax.random.permutation(seeds[8], SEQS).astype(jnp.int32),
    }


loss_scale = 256.0
highest = lax.Precision.HIGHEST

def route_tables(expert_ids, route_share, capacity):
    experts_iota = jnp.arange(EXPERTS, dtype=jnp.int32)
    first_hot = (expert_ids[:, 0:1] == experts_iota[None, :]).astype(jnp.int32)
    second_hot = (expert_ids[:, 1:2] == experts_iota[None, :]).astype(jnp.int32)
    first_rank = lax.optimization_barrier(jnp.sum((jnp.cumsum(first_hot, axis=0) - first_hot) * first_hot, axis=1))
    second_before = jnp.cumsum(second_hot, axis=0) - second_hot + lax.optimization_barrier(jnp.sum(first_hot, axis=0))[None, :]
    second_rank = lax.optimization_barrier(jnp.sum(second_before * second_hot, axis=1))
    route_ranks = jnp.stack([first_rank, second_rank], axis=1).astype(jnp.int32)
    route_kept = route_ranks < capacity
    slot_index = jnp.where(route_kept, expert_ids * capacity + route_ranks, -1).astype(jnp.int32)
    shares = jnp.stack([route_share, 1.0 - route_share], axis=1) * route_kept.astype(jnp.float32)
    slot_iota = jnp.arange(EXPERTS * capacity, dtype=jnp.int32)
    matches = (slot_index[:, :, None] == slot_iota[None, None, :]).astype(jnp.float32)
    picker = lax.optimization_barrier(jnp.sum(matches, axis=1))
    mixing = lax.optimization_barrier(jnp.sum(matches * shares[:, :, None], axis=1))
    return (picker, mixing)

def silu_parts(gate_pre):
    sigmoid_value = jax.nn.sigmoid(gate_pre)
    return (gate_pre * sigmoid_value, sigmoid_value * (1.0 + gate_pre * (1.0 - sigmoid_value)))

def block_sum(lefts, rights):
    group_size = FF // (N_EP // EXPERTS * N_TP)
    group_count = FF // group_size
    row_count = lefts[0].shape[0]
    col_count = rights[0].shape[1]
    left_blocks = tuple((matrix.reshape(row_count, group_count, group_size).transpose(1, 0, 2) for matrix in lefts))
    right_blocks = tuple((matrix.reshape(group_count, group_size, col_count) for matrix in rights))

    def accumulate(running, pieces):
        left_set, right_set = pieces
        partial_sum = jnp.dot(left_set[0], right_set[0], preferred_element_type=jnp.float32)
        for position in range(1, len(left_set)):
            partial_sum = partial_sum + jnp.dot(left_set[position], right_set[position], preferred_element_type=jnp.float32)
        rounded = lax.optimization_barrier(partial_sum.astype(jnp.bfloat16))
        return (running + rounded.astype(jnp.float32), None)
    start_value = jnp.zeros((row_count, col_count), jnp.float32)
    return lax.scan(accumulate, start_value, (left_blocks, right_blocks))[0]

def project(rows_in, weight):
    return lax.dot_general(rows_in, weight, (((1,), (1,)), ((), ())), preferred_element_type=jnp.float32)

def expert_forward(operands):
    rows_in, gate_w, up_w, down_w = operands
    gate_pre = project(rows_in, gate_w)
    up_pre = project(rows_in, up_w)
    silu_value, silu_slope = silu_parts(gate_pre)
    hidden = (silu_value * up_pre).astype(jnp.bfloat16)
    return block_sum((hidden,), (down_w,))

def expert_backward(operands):
    rows_in, grads_in, gate_w, up_w, down_w = operands
    gate_pre = project(rows_in, gate_w)
    up_pre = project(rows_in, up_w)
    silu_value, silu_slope = silu_parts(gate_pre)
    hidden = (silu_value * up_pre).astype(jnp.bfloat16)
    hidden_grad = project(grads_in, down_w)
    gate_grad = (hidden_grad * up_pre * silu_slope).astype(jnp.bfloat16)
    up_grad = (hidden_grad * silu_value).astype(jnp.bfloat16)
    contract = (((0,), (0,)), ((), ()))
    grad_down = lax.dot_general(hidden, grads_in, contract, preferred_element_type=jnp.float32).astype(jnp.bfloat16)
    grad_gate = lax.dot_general(gate_grad, rows_in, contract, preferred_element_type=jnp.float32).astype(jnp.bfloat16)
    grad_up = lax.dot_general(up_grad, rows_in, contract, preferred_element_type=jnp.float32).astype(jnp.bfloat16)
    input_sums = block_sum((gate_grad, up_grad), (gate_w, up_w))
    return (grad_gate, grad_up, grad_down, input_sums)

def to_experts(per_source, capacity):
    width = per_source.shape[2]
    arranged = per_source.reshape(N_EP, EXPERTS, capacity, width).transpose(1, 0, 2, 3)
    return arranged.reshape(EXPERTS, N_EP * capacity, width)

def to_sources(per_expert, capacity):
    width = per_expert.shape[2]
    arranged = per_expert.reshape(EXPERTS, N_EP, capacity, width).transpose(1, 0, 2, 3)
    return arranged.reshape(N_EP, EXPERTS * capacity, width)

def reference(tokens, expert_ids, route_share, w_gate, w_up, w_down, reward_head, upstream, pair_order):
    capacity = TOK_DEV * TOPK // EXPERTS
    token_blocks = tokens.reshape(N_EP, TOK_DEV, D).astype(jnp.float32)
    picker, mixing = jax.vmap(partial(route_tables, capacity=capacity))(expert_ids.reshape(N_EP, TOK_DEV, TOPK), route_share.reshape(N_EP, TOK_DEV))
    gathered = jnp.einsum('pts,ptd->psd', picker, token_blocks, precision=highest)
    slot_inputs = to_experts(gathered.astype(jnp.bfloat16), capacity)
    gate_all = w_gate.reshape(EXPERTS, FF, D)
    up_all = w_up.reshape(EXPERTS, FF, D)
    down_all = w_down.reshape(EXPERTS, FF, D)
    expert_out = lax.map(expert_forward, (slot_inputs, gate_all, up_all, down_all))
    mixed_sum = jnp.einsum('pts,psd->ptd', mixing, to_sources(expert_out, capacity), precision=highest)
    layer_out = (token_blocks + mixed_sum).astype(jnp.bfloat16).reshape(TOKENS, D)
    scores = jnp.dot(layer_out.astype(jnp.float32), reward_head, precision=highest)
    rewards = lax.optimization_barrier(jnp.sum(scores.reshape(SEQS, SEQ_LEN), axis=1)) / math.sqrt(SEQ_LEN)
    seq_iota = jnp.arange(SEQS, dtype=jnp.int32)
    chosen_hot = (pair_order[0::2][:, None] == seq_iota[None, :]).astype(jnp.float32)
    rejected_hot = (pair_order[1::2][:, None] == seq_iota[None, :]).astype(jnp.float32)
    margin = jnp.dot(chosen_hot, rewards, precision=highest) - jnp.dot(rejected_hot, rewards, precision=highest)
    pair_loss = jnp.mean(jax.nn.softplus(-margin))
    pair_weight = jax.nn.sigmoid(-margin)
    seq_coef = jnp.dot(pair_weight, rejected_hot - chosen_hot, precision=highest)
    token_coef = jnp.repeat(seq_coef, SEQ_LEN)
    grad_out = (upstream.astype(jnp.float32) + loss_scale * token_coef[:, None] * reward_head[None, :] / math.sqrt(SEQ_LEN)).astype(jnp.bfloat16)
    grad_blocks = grad_out.reshape(N_EP, TOK_DEV, D).astype(jnp.float32)
    slot_grads = to_experts(jnp.einsum('pts,ptd->psd', mixing, grad_blocks, precision=highest).astype(jnp.bfloat16), capacity)
    grad_gate, grad_up, grad_down, input_sums = lax.map(expert_backward, (slot_inputs, slot_grads, gate_all, up_all, down_all))
    returned = jnp.einsum('pts,psd->ptd', picker, to_sources(input_sums, capacity), precision=highest)
    grad_tokens = (grad_blocks + returned).astype(jnp.bfloat16).reshape(TOKENS, D)
    return (layer_out, rewards, pair_loss, grad_tokens, grad_gate.reshape(EXPERTS * FF, D), grad_up.reshape(EXPERTS * FF, D), grad_down.reshape(EXPERTS * FF, D))
```

```python
import math
from functools import partial

import jax
import jax.numpy as jnp
from jax import lax
from jax.experimental import pallas as pl
from jax.experimental.pallas import tpu as pltpu
from jax.sharding import PartitionSpec as P

EXPERTS = 8
SEQ_LEN = 64


loss_scale = 256.0
highest = lax.Precision.HIGHEST


def route_tables(expert_ids, route_share, capacity):
    experts_iota = jnp.arange(EXPERTS, dtype=jnp.int32)
    first_hot = (expert_ids[:, 0:1] == experts_iota[None, :]).astype(jnp.int32)
    second_hot = (expert_ids[:, 1:2] == experts_iota[None, :]).astype(jnp.int32)
    first_rank = jnp.sum((jnp.cumsum(first_hot, axis=0) - first_hot) * first_hot, axis=1)
    second_before = (
        jnp.cumsum(second_hot, axis=0) - second_hot + jnp.sum(first_hot, axis=0)[None, :]
    )
    second_rank = jnp.sum(second_before * second_hot, axis=1)
    route_ranks = jnp.stack([first_rank, second_rank], axis=1)
    route_kept = route_ranks < capacity
    slot_index = jnp.where(route_kept, expert_ids * capacity + route_ranks, -1)
    shares = jnp.stack([route_share, 1.0 - route_share], axis=1) * route_kept.astype(jnp.float32)
    slot_iota = jnp.arange(EXPERTS * capacity, dtype=jnp.int32)
    matches = (slot_index[:, :, None] == slot_iota[None, None, :]).astype(jnp.float32)
    picker = jnp.sum(matches, axis=1)
    mixing = jnp.sum(matches * shares[:, :, None], axis=1)
    return (picker, mixing)


def silu_parts(gate_pre):
    sigmoid_value = jax.nn.sigmoid(gate_pre)
    return (gate_pre * sigmoid_value, sigmoid_value * (1.0 + gate_pre * (1.0 - sigmoid_value)))


def slot_buffer(picker, source_rows, capacity):
    selected = lax.dot_general(
        picker.astype(jnp.bfloat16),
        source_rows,
        (((0,), (0,)), ((), ())),
        preferred_element_type=jnp.float32,
    )
    return selected.astype(jnp.bfloat16).reshape(EXPERTS, capacity, source_rows.shape[1])


MESH = pl.DeviceIdType.MESH


def remote(src, dst, send_sem, recv_sem, target):
    return pltpu.make_async_remote_copy(
        src_ref=src,
        dst_ref=dst,
        send_sem=send_sem,
        recv_sem=recv_sem,
        device_id=target,
        device_id_type=MESH,
    )


def spread_kernel(
    n_ep, n_tp, tok_ref, ups_ref, meta_ref, head_ref, tok_out, ups_out, meta_out, head_out,
    local_sem, tok_send, ups_send, meta_send, head_send, tp_send,
    tok_recv, ups_recv, meta_recv, head_recv, tp_recv,
):
    q = lax.axis_index("ep")
    t = lax.axis_index("tp")
    width = tok_ref.shape[2]
    replicas = n_ep // tok_ref.shape[0]
    partner = t + 1 - 2 * (t % 2)

    barrier = pltpu.get_barrier_semaphore()
    for k in range(1, n_ep):
        pl.semaphore_signal(barrier, inc=1, device_id=((q + k) % n_ep, t), device_id_type=MESH)
    for k in range(1, n_tp):
        pl.semaphore_signal(barrier, inc=1, device_id=(q, (t + k) % n_tp), device_id_type=MESH)
    pl.semaphore_wait(barrier, n_ep + n_tp - 2)

    def columns(owner):
        return pl.ds(pl.multiple_of(owner * width, 128), width)

    own = q // replicas
    local = [
        pltpu.make_async_copy(tok_ref.at[own], tok_out.at[q, :, columns(t)], local_sem.at[0]),
        pltpu.make_async_copy(ups_ref.at[own], ups_out.at[q], local_sem.at[1]),
        pltpu.make_async_copy(meta_ref.at[own], meta_out.at[q], local_sem.at[2]),
        pltpu.make_async_copy(head_ref, head_out.at[t], local_sem.at[3]),
    ]
    for copy in local:
        copy.start()
    for k in range(1, n_ep):
        to = (q + k) % n_ep
        remote(
            tok_ref.at[to // replicas], tok_out.at[q, :, columns(t)],
            tok_send, tok_recv.at[k], (to, t),
        ).start()
    for k in range(1, n_tp):
        remote(
            head_ref, head_out.at[t], head_send, head_recv.at[k], (q, (t + k) % n_tp)
        ).start()
    for k in range(1, n_ep):
        to = (q + k) % n_ep
        remote(
            meta_ref.at[to // replicas], meta_out.at[q], meta_send, meta_recv.at[k], (to, t)
        ).start()
        remote(
            ups_ref.at[to // replicas], ups_out.at[q], ups_send, ups_recv.at[k], (to, t)
        ).start()

    def hand_on(k, owner, target, row):
        piece = tok_out.at[(q + n_ep - k) % n_ep, :, columns(owner)]
        return remote(piece, piece, tp_send, tp_recv.at[row, k], (q, target))

    def forward(k):
        for j in range(1, n_tp // 2):
            origin = (t + n_tp - 2 * j) % n_tp
            hand_on(k, origin, t, j - 1).wait_recv()
            hand_on(k, origin, partner, n_tp // 2 - 1 + j).start()

    lag = 2
    for k in range(n_ep):
        if k == 0:
            local[0].wait()
        else:
            source = (q + n_ep - k) % n_ep
            remote(
                tok_ref.at[0], tok_out.at[source, :, columns(t)],
                tok_send, tok_recv.at[k], (source, t),
            ).wait_recv()
        for j in range(1, n_tp // 2):
            hand_on(k, t, (t + 2 * j) % n_tp, j - 1).start()
        hand_on(k, t, partner, n_tp // 2 - 1).start()
        if k >= lag:
            forward(k - lag)
    for k in range(max(n_ep - lag, 0), n_ep):
        forward(k)
    for k in range(n_ep):
        hand_on(k, partner, t, n_tp // 2 - 1).wait_recv()
        for j in range(1, n_tp // 2):
            origin = (partner + n_tp - 2 * j) % n_tp
            hand_on(k, origin, t, n_tp // 2 - 1 + j).wait_recv()
    for copy in local[1:]:
        copy.wait()
    for k in range(1, n_tp):
        source = (t + n_tp - k) % n_tp
        remote(head_ref, head_out.at[source], head_send, head_recv.at[k], (q, source)).wait_recv()
    for k in range(1, n_ep):
        source = (q + n_ep - k) % n_ep
        remote(
            meta_ref.at[0], meta_out.at[source], meta_send, meta_recv.at[k], (source, t)
        ).wait_recv()
        remote(
            ups_ref.at[0], ups_out.at[source], ups_send, ups_recv.at[k], (source, t)
        ).wait_recv()

    def drain(sent, sem):
        pltpu.make_async_copy(sent, sent, sem).wait()

    drain(ups_out.at[pl.ds(0, n_ep - 1)], tok_send)
    drain(ups_out.at[pl.ds(0, n_ep - 1)], ups_send)
    drain(meta_out.at[pl.ds(0, n_ep - 1)], meta_send)
    drain(head_out.at[pl.ds(0, n_tp - 1)], head_send)
    drain(tok_out.at[:, :, pl.ds(0, (n_tp - 1) * width)], tp_send)


def spread_slots(tok_buf, ups_buf, meta, head_rows):
    n_ep = lax.axis_size("ep")
    n_tp = lax.axis_size("tp")
    experts, capacity, width = tok_buf.shape
    dma = pltpu.SemaphoreType.DMA
    vmem = pl.BlockSpec(memory_space=pltpu.VMEM)
    return pl.pallas_call(
        partial(spread_kernel, n_ep, n_tp),
        out_shape=(
            jax.ShapeDtypeStruct((n_ep, capacity, n_tp * width), jnp.bfloat16),
            jax.ShapeDtypeStruct((n_ep, capacity, width), jnp.bfloat16),
            jax.ShapeDtypeStruct((n_ep,) + meta.shape[1:], jnp.float32),
            jax.ShapeDtypeStruct((n_tp,) + head_rows.shape, jnp.float32),
        ),
        in_specs=[vmem] * 4,
        out_specs=[vmem] * 4,
        scratch_shapes=[
            dma((4,)), dma, dma, dma, dma, dma,
            dma((n_ep,)), dma((n_ep,)), dma((n_ep,)), dma((n_tp,)), dma((n_tp - 1, n_ep)),
        ],
        compiler_params=pltpu.CompilerParams(collective_id=0, has_side_effects=True),
        name="spread_slots",
    )(tok_buf, ups_buf, meta, head_rows)


def share_kernel(n_ep, n_tp, mine_ref, all_ref, local_sem, send_sem, recv_sem):
    q = lax.axis_index("ep")
    t = lax.axis_index("tp")
    count = n_ep * n_tp
    me = q * n_tp + t
    barrier = pltpu.get_barrier_semaphore()

    def greet(k, carry):
        other = (me + k) % count
        pl.semaphore_signal(
            barrier, inc=1, device_id=(other // n_tp, other % n_tp), device_id_type=MESH
        )
        return carry

    lax.fori_loop(1, count, greet, 0)
    pl.semaphore_wait(barrier, count - 1)
    own = pltpu.make_async_copy(mine_ref, all_ref.at[me], local_sem)
    own.start()

    def send(k, carry):
        other = (me + k) % count
        remote(
            mine_ref, all_ref.at[me], send_sem, recv_sem, (other // n_tp, other % n_tp)
        ).start()
        return carry

    lax.fori_loop(1, count, send, 0)
    own.wait()
    rest = all_ref.at[pl.ds(0, count - 1)]
    pltpu.make_async_copy(rest, rest, recv_sem).wait()
    pltpu.make_async_copy(rest, rest, send_sem).wait()


def share_rows(mine):
    n_ep = lax.axis_size("ep")
    n_tp = lax.axis_size("tp")
    dma = pltpu.SemaphoreType.DMA
    vmem = pl.BlockSpec(memory_space=pltpu.VMEM)
    return pl.pallas_call(
        partial(share_kernel, n_ep, n_tp),
        out_shape=jax.ShapeDtypeStruct((n_ep * n_tp,) + mine.shape, jnp.float32),
        in_specs=[vmem],
        out_specs=vmem,
        scratch_shapes=[dma, dma, dma],
        compiler_params=pltpu.CompilerParams(collective_id=1, has_side_effects=True),
        name="share_rows",
    )(mine)


def return_sums(sums, local_width, replicas, capacity):
    partial_sum = lax.psum_scatter(
        sums,
        "tp",
        scatter_dimension=0,
        tiled=True,
    ).astype(jnp.float32)
    arrived = lax.all_to_all(
        partial_sum.reshape(local_width, -1, capacity).astype(jnp.bfloat16),
        "ep",
        split_axis=1,
        concat_axis=1,
        tiled=True,
    ).astype(jnp.float32)
    grouped = arrived.reshape(local_width, EXPERTS, replicas, capacity)
    return jnp.sum(grouped, axis=2).reshape(local_width, EXPERTS * capacity)


def per_device(
    tokens, expert_ids, route_share, w_gate, w_up, w_down, reward_head, upstream, pair_order
):
    tok_count, local_width = tokens.shape
    capacity = tok_count * expert_ids.shape[1] // EXPERTS
    n_ep = lax.axis_size("ep")
    replicas = n_ep // EXPERTS
    seq_local = tok_count // SEQ_LEN
    seq_total = pair_order.shape[0]
    seq_scale = loss_scale / math.sqrt(SEQ_LEN)
    picker, mixing = route_tables(expert_ids, route_share, capacity)
    tok_buf = slot_buffer(picker, tokens, capacity)
    ups_buf = slot_buffer(picker, upstream, capacity)
    seq_share = jnp.sum(mixing.reshape(seq_local, SEQ_LEN, EXPERTS, capacity), axis=1)
    meta = jnp.zeros((EXPERTS, 8 * pl.cdiv(seq_local, 8), 128 * pl.cdiv(capacity, 128)), jnp.float32)
    meta = meta.at[:, :seq_local, :capacity].set(seq_share.transpose(1, 0, 2))
    slot_rows, ups_part, meta_all, head_all = spread_slots(
        tok_buf, ups_buf, meta, reward_head.reshape(-1, 128)
    )
    width = slot_rows.shape[2]
    slot_rows = slot_rows.reshape(-1, width)
    ups_rows = lax.all_gather(ups_part, "tp", axis=2, tiled=True).reshape(-1, width)
    head_full = head_all.reshape(width)
    slot_meta = meta_all[:, :seq_local, :capacity]

    rows_by_cols = (((1,), (1,)), ((), ()))
    gate_pre = lax.dot_general(slot_rows, w_gate, rows_by_cols, preferred_element_type=jnp.float32)
    up_pre = lax.dot_general(slot_rows, w_up, rows_by_cols, preferred_element_type=jnp.float32)
    silu_value, silu_slope = silu_parts(gate_pre)
    hidden = (silu_value * up_pre).astype(jnp.bfloat16)

    def down_term(first_row, row_count):
        return lax.dot_general(
            w_down, hidden, (((0,), (1,)), ((), ())), preferred_element_type=jnp.float32
        )

    down_sums = down_term(0, 0).astype(jnp.bfloat16)
    down_sums, ups_rows, head_full = lax.optimization_barrier((down_sums, ups_rows, head_full))
    expert_sums = return_sums(down_sums, local_width, replicas, capacity)

    ups_cols = lax.dot_general(ups_rows, w_down, rows_by_cols, preferred_element_type=jnp.float32)
    head_parts = []
    head_rest = head_full
    for _ in range(3):
        part = lax.reduce_precision(head_rest, 8, 7)
        head_parts.append(part.astype(jnp.bfloat16))
        head_rest = head_rest - part
    head_cols = jnp.sum(
        lax.dot_general(
            jnp.stack(head_parts), w_down, rows_by_cols, preferred_element_type=jnp.float32
        ),
        axis=0,
    )

    slot_scores = jnp.sum(hidden.astype(jnp.float32) * head_cols[None, :], axis=1)
    expert_part = jnp.sum(slot_meta * slot_scores.reshape(n_ep, 1, capacity), axis=2).reshape(-1)
    own_scores = jnp.sum(tokens.astype(jnp.float32) * reward_head[None, :], axis=1)
    own_part = jnp.sum(own_scores.reshape(seq_local, SEQ_LEN), axis=1)
    offset = lax.axis_index("ep") * seq_local
    placed = lax.dynamic_update_slice(jnp.zeros((seq_total,), jnp.float32), own_part, (offset,))
    lanes = 1024 * pl.cdiv(seq_total, 1024)
    mine = jnp.pad(placed + expert_part, (0, lanes - seq_total)).reshape(-1, 128)
    gathered = share_rows(mine)
    rewards = jnp.sum(gathered, axis=0).reshape(-1)[:seq_total] / math.sqrt(SEQ_LEN)

    seq_iota = jnp.arange(seq_total, dtype=jnp.int32)
    chosen_hot = (pair_order[0::2][:, None] == seq_iota[None, :]).astype(jnp.float32)
    rejected_hot = (pair_order[1::2][:, None] == seq_iota[None, :]).astype(jnp.float32)
    margin = jnp.sum((chosen_hot - rejected_hot) * rewards[None, :], axis=1)
    pair_loss = jnp.mean(jax.nn.softplus(-margin))
    pair_weight = jax.nn.sigmoid(-margin)
    seq_coef = jnp.sum(pair_weight[:, None] * (rejected_hot - chosen_hot), axis=0)
    token_coef = jnp.repeat(lax.dynamic_slice_in_dim(seq_coef, offset, seq_local), SEQ_LEN)
    grad_out = (
        upstream.astype(jnp.float32) + seq_scale * token_coef[:, None] * reward_head[None, :]
    ).astype(jnp.bfloat16)

    slot_share = jnp.sum(slot_meta, axis=1).reshape(-1, 1)
    coef_of = seq_coef.reshape(n_ep, seq_local, 1)
    slot_coef = seq_scale * jnp.sum(jnp.where(slot_meta > 0.0, coef_of, 0.0), axis=1).reshape(-1, 1)
    slot_out = (ups_rows.astype(jnp.float32) + slot_coef * head_full[None, :]).astype(jnp.bfloat16)
    grad_slots = (slot_share * slot_out.astype(jnp.float32)).astype(jnp.bfloat16)
    hidden_grad = slot_share * (ups_cols + slot_coef * head_cols[None, :])
    gate_grad = (hidden_grad * up_pre * silu_slope).astype(jnp.bfloat16)
    up_grad = (hidden_grad * silu_value).astype(jnp.bfloat16)

    def input_term(first_row, row_count):
        across = (((0,), (1,)), ((), ()))
        return lax.dot_general(
            w_gate, gate_grad, across, preferred_element_type=jnp.float32
        ) + lax.dot_general(w_up, up_grad, across, preferred_element_type=jnp.float32)

    term_sums = input_term(0, 0).astype(jnp.bfloat16)
    term_sums, gate_grad, up_grad, grad_slots = lax.optimization_barrier(
        (term_sums, gate_grad, up_grad, grad_slots)
    )
    input_sums = return_sums(term_sums, local_width, replicas, capacity)

    over_slots = (((0,), (0,)), ((), ()))
    grad_down = lax.dot_general(
        hidden, grad_slots, over_slots, preferred_element_type=jnp.float32
    ).astype(jnp.bfloat16)
    grad_gate = lax.dot_general(
        gate_grad, slot_rows, over_slots, preferred_element_type=jnp.float32
    ).astype(jnp.bfloat16)
    grad_up = lax.dot_general(
        up_grad, slot_rows, over_slots, preferred_element_type=jnp.float32
    ).astype(jnp.bfloat16)

    mixed_sum = lax.dot_general(
        mixing, expert_sums, rows_by_cols, precision=highest, preferred_element_type=jnp.float32
    )
    layer_out = (tokens.astype(jnp.float32) + mixed_sum).astype(jnp.bfloat16)
    returned = lax.dot_general(
        picker, input_sums, rows_by_cols, precision=highest, preferred_element_type=jnp.float32
    )
    grad_tokens = (grad_out.astype(jnp.float32) + returned).astype(jnp.bfloat16)
    return (layer_out, rewards, pair_loss, grad_tokens, grad_gate, grad_up, grad_down)


def solution(mesh):
    in_specs = (
        P("ep", "tp"),
        P("ep", None),
        P("ep"),
        P(("ep", "tp"), None),
        P(("ep", "tp"), None),
        P(("ep", "tp"), None),
        P("tp"),
        P("ep", "tp"),
        P(),
    )
    out_specs = (
        P("ep", "tp"),
        P(),
        P(),
        P("ep", "tp"),
        P(("ep", "tp"), None),
        P(("ep", "tp"), None),
        P(("ep", "tp"), None),
    )
    return jax.shard_map(
        per_device, mesh=mesh, in_specs=in_specs, out_specs=out_specs, check_vma=False
    )
```
